32 devices in a mesh: data: 2 (over x), seq: 4 (over z), dap: 4 (over y, core).
Axes of the slice: x: 2, y: 2, z: 4, core: 2. Of those that a mesh axis runs over, the one named last changes fastest.
Arguments:
- msa_act: bfloat16 [1024, 512, 64], P(('data', 'seq', 'dap')), parts along dimension 0
- msa_mask: int32 [1024, 512], P(('data', 'seq', 'dap')), parts along dimension 0
- pair_act: float32 [1024, 512, 128], P(('data', 'dap')), parts along dimension 0
- ln_gamma: bfloat16 [64], replicated
- ln_beta: bfloat16 [64], replicated
- w_a: bfloat16 [64, 32], replicated
- b_a: bfloat16 [32], replicated
- w_b: bfloat16 [64, 32], replicated
- b_b: bfloat16 [32], replicated
- w_out: bfloat16 [1024, 128], replicated
- b_out: bfloat16 [128], replicated
Outputs:
- output: float32 [1024, 512, 128], P(('data', 'dap')), parts along dimension 0
There are 2 independent parts. The reference program is written for one: setup_inputs(seed, part) draws one part's arguments, and reference() takes and returns one part's arrays. A program takes and returns all parts, laid end to end along the dimension named above; an argument that names none is the same for every part.
All inputs are finite; a program needn't handle non-finite values.
Results may differ from the reference program's by a relative error of at most 0.0123679.
Values are sent between devices in bfloat16 or wider.
A program may use at most 1 GiB of HBM per device.

```python
import jax
import jax.numpy as jnp
from jax import lax

NUM_SEQS = 512
NUM_RES = 512
MSA_DIM = 64
PAIR_DIM = 128
HIDDEN = 32
SEQ_BLOCK = 8


def draw_mask(level_key, draw_key):
    levels = jax.random.randint(level_key, (NUM_SEQS, 1), 0, 17)
    draws = jax.random.randint(draw_key, (NUM_SEQS, NUM_RES), 0, 16)
    first_row = (jnp.arange(NUM_SEQS) == 0)[:, None]
    return jnp.where(first_row | (draws < levels), 1, 0).astype(jnp.int32)


def setup_inputs(seed: int = 0, part: int = 0) -> dict:
    root = jax.random.key(seed)
    shared = jax.random.split(root, 8)
    own = jax.random.split(jax.random.fold_in(root, part), 4)
    common = NUM_SEQS ** -0.25

    def normal(key, shape):
        return jax.random.normal(key, shape, jnp.float32)

    msa_act = normal(own[0], (NUM_SEQS, NUM_RES, MSA_DIM)).astype(jnp.bfloat16)
    msa_mask = draw_mask(own[1], own[2])
    pair_act = normal(own[3], (NUM_RES, NUM_RES, PAIR_DIM))
    ln_gamma = (1.0 + 0.5 * normal(shared[0], (MSA_DIM,))).astype(jnp.bfloat16)
    ln_beta = (0.7 * common * normal(shared[1], (MSA_DIM,))).astype(jnp.bfloat16)
    w_a = (normal(shared[2], (MSA_DIM, HIDDEN)) * MSA_DIM ** -0.5).astype(jnp.bfloat16)
    b_a = (0.7 * common * normal(shared[3], (HIDDEN,))).astype(jnp.bfloat16)
    w_b = (normal(shared[4], (MSA_DIM, HIDDEN)) * MSA_DIM ** -0.5).astype(jnp.bfloat16)
    b_b = (0.7 * common * normal(shared[5], (HIDDEN,))).astype(jnp.bfloat16)
    w_out = (normal(shared[6], (HIDDEN * HIDDEN, PAIR_DIM)) * (0.7 * NUM_SEQS ** 0.5 / HIDDEN)).astype(jnp.bfloat16)
    b_out = (0.5 * NUM_SEQS * normal(shared[7], (PAIR_DIM,))).astype(jnp.bfloat16)
    return {'msa_act': msa_act, 'msa_mask': msa_mask, 'pair_act': pair_act, 'ln_gamma': ln_gamma, 'ln_beta': ln_beta, 'w_a': w_a, 'b_a': b_a, 'w_b': w_b, 'b_b': b_b, 'w_out': w_out, 'b_out': b_out}


def layer_norm(msa_blk, ln_gamma, ln_beta):
    values = msa_blk.astype(jnp.float32)
    row_mean = jnp.mean(values, axis=-1, keepdims=True)
    centered = values - row_mean
    variance = jnp.mean(centered * centered, axis=-1, keepdims=True)
    normed = centered * lax.rsqrt(variance + 1e-5)
    return (normed * ln_gamma.astype(jnp.float32) + ln_beta.astype(jnp.float32)).astype(jnp.bfloat16)


def project(normed, weight, bias_vec, weight_mask):
    summed = jnp.einsum('snk,kc->snc', normed.astype(jnp.float32), weight.astype(jnp.float32))
    return ((summed + bias_vec.astype(jnp.float32)) * weight_mask[..., None]).astype(jnp.bfloat16)


def reference(msa_act, msa_mask, pair_act, ln_gamma, ln_beta, w_a, b_a, w_b, b_b, w_out, b_out):
    w_cube = w_out.astype(jnp.float32).reshape(HIDDEN, HIDDEN, PAIR_DIM)
    num_blocks = NUM_SEQS // SEQ_BLOCK
    msa_blocks = msa_act.reshape(num_blocks, SEQ_BLOCK, NUM_RES, MSA_DIM)
    mask_blocks = msa_mask.reshape(num_blocks, SEQ_BLOCK, NUM_RES)

    def body(carry, block_in):
        sum_r, sum_n = carry
        msa_blk, mask_blk = block_in
        seq_keep = mask_blk.astype(jnp.float32)
        normed = layer_norm(msa_blk, ln_gamma, ln_beta)
        left = project(normed, w_a, b_a, seq_keep)
        right = project(normed, w_b, b_b, seq_keep)
        lifted = jnp.einsum('sic,cde->side', left.astype(jnp.float32), w_cube).astype(jnp.bfloat16)
        sum_r = sum_r + jnp.einsum('side,sjd->ije', lifted.astype(jnp.float32), right.astype(jnp.float32))
        sum_n = sum_n + jnp.einsum('si,sj->ij', seq_keep, seq_keep)
        return (sum_r, sum_n), None

    start_state = (jnp.zeros((NUM_RES, NUM_RES, PAIR_DIM), jnp.float32), jnp.zeros((NUM_RES, NUM_RES), jnp.float32))
    (total_r, total_n), _ = lax.scan(body, start_state, (msa_blocks, mask_blocks))
    return pair_act + (total_r + b_out.astype(jnp.float32)) / (1e-3 + total_n[..., None])
```

```python
import functools
import jax
import jax.numpy as jnp
from jax import lax
from jax.sharding import PartitionSpec as P
from jax.experimental import pallas as pl
from jax.experimental.pallas import tpu as pltpu

F32 = jnp.float32
BF16 = jnp.bfloat16
VMEM_LIMIT = 60 * 1024 * 1024
S_STEP = 16
I_STEP = 16
J_STEP = 128


def project_kernel(msa_ref, mask_ref, gamma_ref, beta_ref, weight_ref, bias_ref, out_ref, tmp_ref):
    res, width = msa_ref.shape[1:]
    for s in range(S_STEP):
        x = msa_ref[s].astype(F32).T
        mean = jnp.sum(x, axis=0, keepdims=True) * (1.0 / width)
        centered = x - mean
        var = jnp.sum(centered * centered, axis=0, keepdims=True) * (1.0 / width)
        normed = centered * lax.rsqrt(var + 1e-5)
        normed = (normed * gamma_ref[...] + beta_ref[...]).astype(BF16)
        proj = jnp.dot(weight_ref[...], normed, preferred_element_type=F32) + bias_ref[...]
        tmp_ref[s] = proj * mask_ref[s:s + 1, :].astype(F32)
    half = out_ref.shape[1] - 1
    for g in range(2 * half // 8):
        flat = jnp.transpose(tmp_ref[:, g * 8:g * 8 + 8, :], (1, 0, 2)).astype(BF16)
        part, base = divmod(g * 8, half)
        out_ref[part, base:base + 8] = flat
    keep = mask_ref[...].astype(F32).astype(BF16)
    out_ref[0, half] = keep
    out_ref[1, half] = keep


def project(msa, mask, gamma, beta, weight, bias):
    seqs, res, width = msa.shape
    chans = weight.shape[0]
    return pl.pallas_call(
        project_kernel,
        grid=(seqs // S_STEP,),
        in_specs=[
            pl.BlockSpec((S_STEP, res, width), lambda g: (g, 0, 0)),
            pl.BlockSpec((S_STEP, res), lambda g: (g, 0)),
            pl.BlockSpec((width, 1), lambda g: (0, 0)),
            pl.BlockSpec((width, 1), lambda g: (0, 0)),
            pl.BlockSpec((chans, width), lambda g: (0, 0)),
            pl.BlockSpec((chans, 1), lambda g: (0, 0)),
        ],
        out_specs=pl.BlockSpec((2, chans // 2 + 1, S_STEP, res), lambda g: (0, 0, g, 0)),
        out_shape=jax.ShapeDtypeStruct((2, chans // 2 + 1, seqs, res), BF16),
        scratch_shapes=[pltpu.VMEM((S_STEP, chans, res), F32)],
        compiler_params=pltpu.CompilerParams(vmem_limit_bytes=VMEM_LIMIT),
        name='project',
    )(msa, mask, gamma, beta, weight, bias)


def turn_kernel(row_ref, left_ref, out_ref, keep_ref, tmp_ref):
    src, chans, seqs, rows = left_ref.shape
    for c in range(chans):
        block = left_ref[:, c].reshape(src * seqs, rows).astype(F32).T
        if c == chans - 1:
            keep_ref[...] = block.astype(BF16)
        else:
            tmp_ref[c] = block

    @pl.loop(0, rows // 8)
    def _(g):
        start = pl.multiple_of(g * 8, 8)
        block = jnp.transpose(tmp_ref[:, pl.ds(start, 8), :], (1, 0, 2)).astype(BF16)
        out_ref[pl.ds(start, 8)] = block


def turn(row_block, left):
    src, _, chans, seqs, res = left.shape
    rows = res // 4
    total = src * seqs
    return pl.pallas_call(
        turn_kernel,
        grid_spec=pltpu.PrefetchScalarGridSpec(
            num_scalar_prefetch=1,
            grid=(1,),
            in_specs=[pl.BlockSpec((src, None, chans, seqs, rows), lambda g, row: (0, 0, 0, 0, row[0]))],
            out_specs=[
                pl.BlockSpec((rows, chans - 1, total), lambda g, row: (0, 0, 0)),
                pl.BlockSpec((rows, total), lambda g, row: (0, 0)),
            ],
            scratch_shapes=[pltpu.VMEM((chans - 1, rows, total), F32)],
        ),
        out_shape=[
            jax.ShapeDtypeStruct((rows, chans - 1, total), BF16),
            jax.ShapeDtypeStruct((rows, total), BF16),
        ],
        compiler_params=pltpu.CompilerParams(vmem_limit_bytes=VMEM_LIMIT),
        name='turn',
    )(row_block, left)


def product_kernel(left_ref, keep_ref, right_ref, weight_ref, bias_ref, pair_ref, out_ref, outer_ref, scale_ref):
    rows, chans, total = left_ref.shape
    cols = right_ref.shape[-1]
    left = left_ref[...].reshape(rows * chans, total)
    count = jnp.dot(keep_ref[...], right_ref[:, chans].reshape(total, cols), preferred_element_type=F32)
    scale_ref[...] = 1.0 / (1e-3 + count)

    for g in range(chans // 4):
        slab = [right_ref[:, g * 4 + k].reshape(total, cols) for k in range(4)]
        rhs = jnp.concatenate(slab, axis=1)
        for m in range(rows // 8):
            part = left[m * 8 * chans:(m + 1) * 8 * chans]
            prod = jnp.dot(part, rhs, preferred_element_type=F32).astype(BF16)
            for k in range(4):
                at = (g * 4 + k) * chans
                for i in range(8):
                    outer_ref[m * 4 + i // 2, at:at + chans, (i % 2) * cols:(i % 2 + 1) * cols] = (
                        prod[i * chans:(i + 1) * chans, k * cols:(k + 1) * cols])
    for h in range(rows // 2):
        lifted = jnp.dot(weight_ref[...], outer_ref[h], preferred_element_type=F32)
        for k in range(2):
            part = lifted[:, k * cols:(k + 1) * cols] + bias_ref[...]
            part = part * scale_ref[h * 2 + k:h * 2 + k + 1, :]
            out_ref[h * 2 + k] = pair_ref[h * 2 + k] + part.T


def product(left, keep, right, weight, bias, pair):
    rows, chans, total = left.shape
    src, _, _, seqs, res = right.shape
    width = weight.shape[0]
    return pl.pallas_call(
        product_kernel,
        grid=(res // J_STEP, rows // I_STEP),
        in_specs=[
            pl.BlockSpec((I_STEP, chans, total), lambda q, g: (g, 0, 0)),
            pl.BlockSpec((I_STEP, total), lambda q, g: (g, 0)),
            pl.BlockSpec((src, None, chans + 1, seqs, J_STEP), lambda q, g: (0, 1, 0, 0, q)),
            pl.BlockSpec(weight.shape, lambda q, g: (0, 0)),
            pl.BlockSpec(bias.shape, lambda q, g: (0, 0)),
            pl.BlockSpec((I_STEP, J_STEP, width), lambda q, g: (g, q, 0)),
        ],
        out_specs=pl.BlockSpec((I_STEP, J_STEP, width), lambda q, g: (g, q, 0)),
        out_shape=jax.ShapeDtypeStruct(pair.shape, F32),
        scratch_shapes=[pltpu.VMEM((I_STEP // 2, chans * chans, 2 * J_STEP), BF16), pltpu.VMEM((I_STEP, J_STEP), F32)],
        compiler_params=pltpu.CompilerParams(vmem_limit_bytes=VMEM_LIMIT),
        name='product',
    )(left, keep, right, weight, bias, pair)


def solution(mesh):
    msa_spec = P(('data', 'seq', 'dap'), None, None)
    mask_spec = P(('data', 'seq', 'dap'), None)
    pair_spec = P(('data', 'dap'), None, None)

    def device_step(msa, mask, pair, ln_gamma, ln_beta, w_a, b_a, w_b, b_b, w_out, b_out):
        hidden = w_a.shape[1]
        width = w_out.shape[1]
        res = msa.shape[1]
        weight = jnp.concatenate([w_a, w_b], axis=1).T
        bias = jnp.concatenate([b_a, b_b]).astype(F32)[:, None]
        both = project(msa, mask, ln_gamma.astype(F32)[:, None], ln_beta.astype(F32)[:, None], weight, bias)
        lift = w_out.reshape(hidden, hidden, width).transpose(2, 1, 0).reshape(width, hidden * hidden)
        bias_col = jnp.broadcast_to(b_out.astype(F32)[:, None], (width, J_STEP))
        gathered = lax.all_gather(both, ('seq', 'dap'))
        row_block = lax.axis_index('dap').reshape(1).astype(jnp.int32)
        left, keep = turn(row_block, gathered)
        return product(left, keep, gathered, lift, bias_col, pair)

    return jax.shard_map(device_step, mesh=mesh, in_specs=(msa_spec, mask_spec, pair_spec, P(), P(), P(), P(), P(), P(), P(), P()), out_specs=pair_spec, check_vma=False)
```

```python
import functools
import jax
import jax.numpy as jnp
from jax import lax
from jax.sharding import PartitionSpec as P
from jax.experimental import pallas as pl
from jax.experimental.pallas import tpu as pltpu

F32 = jnp.float32
BF16 = jnp.bfloat16
VMEM_LIMIT = 60 * 1024 * 1024
S_STEP = 16
I_STEP = 16
J_STEP = 128
MESH = pl.DeviceIdType.MESH
EARLY = 2


def project_kernel(msa_ref, mask_ref, gamma_ref, beta_ref, weight_ref, bias_ref, out_ref, tmp_ref):
    res, width = msa_ref.shape[1:]
    for s in range(S_STEP):
        x = msa_ref[s].astype(F32).T
        mean = jnp.sum(x, axis=0, keepdims=True) * (1.0 / width)
        centered = x - mean
        var = jnp.sum(centered * centered, axis=0, keepdims=True) * (1.0 / width)
        normed = centered * lax.rsqrt(var + 1e-5)
        normed = (normed * gamma_ref[...] + beta_ref[...]).astype(BF16)
        proj = jnp.dot(weight_ref[...], normed, preferred_element_type=F32) + bias_ref[...]
        tmp_ref[s] = proj * mask_ref[s:s + 1, :].astype(F32)
    half = out_ref.shape[2] - 1
    for g in range(2 * half // 8):
        flat = jnp.transpose(tmp_ref[:, g * 8:g * 8 + 8, :], (1, 0, 2)).astype(BF16)
        part, base = divmod(g * 8, half)
        for k in range(out_ref.shape[1]):
            out_ref[part, k, base:base + 8] = flat[:, :, k * J_STEP:(k + 1) * J_STEP]
    keep = mask_ref[...].astype(F32).astype(BF16)
    for k in range(out_ref.shape[1]):
        out_ref[0, k, half] = keep[:, k * J_STEP:(k + 1) * J_STEP]
        out_ref[1, k, half] = keep[:, k * J_STEP:(k + 1) * J_STEP]


def project(msa, mask, gamma, beta, weight, bias):
    seqs, res, width = msa.shape
    chans = weight.shape[0]
    return pl.pallas_call(
        project_kernel,
        grid=(seqs // S_STEP,),
        in_specs=[
            pl.BlockSpec((S_STEP, res, width), lambda g: (g, 0, 0)),
            pl.BlockSpec((S_STEP, res), lambda g: (g, 0)),
            pl.BlockSpec((width, 1), lambda g: (0, 0)),
            pl.BlockSpec((width, 1), lambda g: (0, 0)),
            pl.BlockSpec((chans, width), lambda g: (0, 0)),
            pl.BlockSpec((chans, 1), lambda g: (0, 0)),
        ],
        out_specs=pl.BlockSpec((2, res // J_STEP, chans // 2 + 1, S_STEP, J_STEP), lambda g: (0, 0, 0, g, 0)),
        out_shape=jax.ShapeDtypeStruct((2, res // J_STEP, chans // 2 + 1, seqs, J_STEP), BF16),
        scratch_shapes=[pltpu.VMEM((S_STEP, chans, res), F32)],
        compiler_params=pltpu.CompilerParams(vmem_limit_bytes=VMEM_LIMIT),
        name='project',
    )(msa, mask, gamma, beta, weight, bias)


def multiply(left, keep, right, weight, bias, outer_ref, scale_ref, emit):
    total = left.shape[-1]
    src, chans, seqs, cols = right.shape
    chans = chans - 1
    rows = left.shape[0] // chans
    count = jnp.dot(keep, right[:, chans].reshape(total, cols), preferred_element_type=F32)
    scale_ref[...] = 1.0 / (1e-3 + count)
    for g in range(chans // 4):
        slab = [right[:, g * 4 + k].reshape(total, cols) for k in range(4)]
        rhs = jnp.concatenate(slab, axis=1)
        for m in range(rows // 8):
            part = left[m * 8 * chans:(m + 1) * 8 * chans, :]
            prod = jnp.dot(part, rhs, preferred_element_type=F32).astype(BF16)
            for k in range(4):
                at = (g * 4 + k) * chans
                for i in range(8):
                    outer_ref[m * 4 + i // 2, at:at + chans, (i % 2) * cols:(i % 2 + 1) * cols] = (
                        prod[i * chans:(i + 1) * chans, k * cols:(k + 1) * cols])
    for h in range(rows // 2):
        lifted = jnp.dot(weight[...], outer_ref[h], preferred_element_type=F32)
        for k in range(2):
            part = lifted[:, k * cols:(k + 1) * cols] + bias[...]
            part = part * scale_ref[h * 2 + k:h * 2 + k + 1, :]
            emit(h * 2 + k, part.T)


def exchange_kernel(both, lift, bias, pair, x_out, bg, ag, left_out, keep_out,
                    left_vm, keep_vm, tmp, araw, bvm, outer, scale, pbuf, obuf, stage,
                    zs, zr, ys, yr, cs, cr, ss, sr, ls, asem, bsem, psem, osem, esem):
    z = lax.axis_index('seq')
    dap = lax.axis_index('dap')
    core = dap + 1 - 2 * lax.rem(dap, 2)
    far = lax.rem(dap + 2, 4)
    diag = lax.rem(core + 2, 4)
    me = z * 4 + dap
    blocks = both.shape[1]

    def remote(src, dst, send, recv, **target):
        return pltpu.make_async_remote_copy(src_ref=src, dst_ref=dst, send_sem=send, recv_sem=recv,
                                            device_id=target, device_id_type=MESH)

    def piece(item, plane):
        return ag.at[plane] if item == 1 else bg.at[max(item - 1, 0), plane * 4 + dap]

    def out_ok(way, h):
        return (z < 3) & (z >= h - 1) if way == 0 else (z > 0) & (z <= 4 - h)

    def in_ok(way, h):
        return z >= h if way == 0 else z + h <= 3

    def z_send(item, way, h):
        sign = 1 - 2 * way
        plane = z - sign * (h - 1)
        src = both.at[1, max(item - 1, 0)] if h == 1 and item != 1 else piece(item, plane)
        return remote(src, piece(item, plane), zs.at[way, item, h - 1], zr.at[way, item, h - 1], seq=z + sign)

    def z_land(item, way, h):
        sign = 1 - 2 * way
        at = piece(item, z - sign * h)
        return remote(at, at, zs.at[way, item, h - 1], zr.at[way, item, h - 1], seq=z - sign)

    def y_send(q, plane, own):
        at = bg.at[q, plane * 4 + dap]
        return remote(both.at[1, q] if own else at, at, ys.at[q, plane], yr.at[q, plane], dap=far)

    def y_land(q, plane):
        at = bg.at[q, plane * 4 + far]
        return remote(at, at, ys.at[q, plane], yr.at[q, plane], dap=far)

    def c_send(q, plane, which, own):
        at = bg.at[q, plane * 4 + (far if which else dap)]
        return remote(both.at[1, q] if own else at, at, cs.at[q, plane, which], cr.at[q, plane, which], dap=core)

    def c_land(q, plane, which):
        at = bg.at[q, plane * 4 + (diag if which else core)]
        return remote(at, at, cs.at[q, plane, which], cr.at[q, plane, which], dap=core)

    def begin(item):
        for way in range(2):
            @pl.when(out_ok(way, 1))
            def _():
                z_send(item, way, 1).start()
        if item != 1:
            q = max(item - 1, 0)
            y_send(q, z, True).start()
            c_send(q, z, 0, True).start()

    def arrive(item, h):
        for way in range(2):
            @pl.when(in_ok(way, h))
            def _():
                z_land(item, way, h).wait_recv()
            if h < 3:
                @pl.when(out_ok(way, h + 1))
                def _():
                    z_send(item, way, h + 1).start()
            if item != 1:
                @pl.when(in_ok(way, h))
                def _():
                    q = max(item - 1, 0)
                    plane = z - (1 - 2 * way) * h
                    y_send(q, plane, False).start()
                    c_send(q, plane, 0, False).start()

    def relay(q, h):
        if h == 0:
            y_land(q, z).wait_recv()
            c_send(q, z, 1, False).start()
        else:
            for way in range(2):
                @pl.when(in_ok(way, h))
                def _():
                    plane = z - (1 - 2 * way) * h
                    y_land(q, plane).wait_recv()
                    c_send(q, plane, 1, False).start()

    def settle(q):
        for plane in range(4):
            for which in range(2):
                c_land(q, plane, which).wait_recv()

    def turn(low, high):
        @pl.loop(0, 4)
        def _(plane):
            gap = jnp.abs(plane - z)

            @pl.when((gap >= low) & (gap <= high))
            def _():
                load = pltpu.make_async_copy(ag.at[plane], araw, asem)
                load.start()
                load.wait()
                lanes = pl.ds(pl.multiple_of(plane * 128, 128), 128)
                chans = araw.shape[1]
                for c in range(chans):
                    block = araw[:, c].reshape(128, 128).astype(F32).T
                    if c == chans - 1:
                        keep_vm[:, lanes] = block.astype(BF16)
                    else:
                        tmp[c] = block

                @pl.loop(0, 16)
                def _(k):
                    start = pl.multiple_of(k * 8, 8)
                    block = jnp.transpose(tmp[:, pl.ds(start, 8), :], (1, 0, 2)).reshape(256, 128)
                    row = pl.multiple_of(lax.rem(k, 2) * 256, 256)
                    left_vm[k // 2, pl.ds(row, 256), lanes] = block.astype(BF16)

    barrier = pltpu.get_barrier_semaphore()
    for other in (core, far, diag):
        pl.semaphore_signal(barrier, inc=1, device_id={'dap': other}, device_id_type=MESH)
    for way in range(2):
        @pl.when(out_ok(way, 1))
        def _():
            pl.semaphore_signal(barrier, inc=1, device_id={'seq': z + 1 - 2 * way}, device_id_type=MESH)
    inner = (z > 0) & (z < 3)

    @pl.when(inner)
    def _():
        pl.semaphore_wait(barrier, 5)

    @pl.when(jnp.logical_not(inner))
    def _():
        pl.semaphore_wait(barrier, 4)

    swaps = [remote(both.at[0, other], ag.at[z, dap], ss.at[k], sr.at[k], dap=other)
             for k, other in enumerate((core, far, diag))]
    for k in (1, 2, 0):
        swaps[k].start()
    begin(0)
    loads = [pltpu.make_async_copy(both.at[1, q], stage.at[q], ls.at[q]) for q in range(blocks)]
    loads.append(pltpu.make_async_copy(both.at[0, dap], stage.at[blocks], ls.at[blocks]))
    for load in loads:
        load.start()
    for load in loads:
        load.wait()
    puts = [pltpu.make_async_copy(stage.at[q], bg.at[q, me], ls.at[q]) for q in range(blocks)]
    puts.append(pltpu.make_async_copy(stage.at[blocks], ag.at[z, dap], ls.at[blocks]))
    for put in puts:
        put.start()
    for put in puts:
        put.wait()
    for k, other in enumerate((core, far, diag)):
        at = ag.at[z, other]
        remote(at, at, ss.at[k], sr.at[k], dap=other).wait_recv()
    begin(1)
    arrive(0, 1)
    relay(0, 0)
    arrive(0, 2)
    relay(0, 1)
    arrive(1, 1)
    begin(2)
    arrive(0, 3)
    relay(0, 2)
    turn(0, 1)
    arrive(1, 2)
    arrive(2, 1)
    begin(3)
    relay(0, 3)
    settle(0)
    first = pltpu.make_async_copy(bg.at[0], bvm.at[0], bsem.at[0])
    first.start()
    turn(2, 2)
    arrive(1, 3)
    turn(3, 3)
    first.wait()

    steps = EARLY * 8

    def pair_load(t):
        return pltpu.make_async_copy(pair.at[pl.ds(pl.multiple_of(lax.rem(t, 8) * I_STEP, I_STEP), I_STEP), t // 8],
                                     pbuf.at[lax.rem(t, 2)], psem.at[lax.rem(t, 2)])

    def out_put(t):
        return pltpu.make_async_copy(obuf.at[lax.rem(t, 2)],
                                     x_out.at[pl.ds(pl.multiple_of(lax.rem(t, 8) * I_STEP, I_STEP), I_STEP), t // 8],
                                     osem.at[lax.rem(t, 2)])

    exports = [pltpu.make_async_copy(left_vm, left_out, esem.at[0]), pltpu.make_async_copy(keep_vm, keep_out, esem.at[1])]
    for export in exports:
        export.start()
    pair_load(0).start()

    events = {
        0: lambda: relay(1, 0),
        1: lambda: (arrive(2, 2), relay(1, 1)),
        3: lambda: (arrive(3, 1), begin(4)),
        4: lambda: (arrive(2, 3), relay(1, 2)),
        6: lambda: (arrive(3, 2), relay(1, 3), relay(2, 0)),
        7: lambda: (settle(1), pltpu.make_async_copy(bg.at[1], bvm.at[1], bsem.at[1]).start()),
        8: lambda: (pltpu.make_async_copy(bg.at[1], bvm.at[1], bsem.at[1]).wait(), relay(2, 1)),
        9: lambda: arrive(4, 1),
        10: lambda: (arrive(3, 3), relay(2, 2)),
        12: lambda: (arrive(4, 2), relay(2, 3), relay(3, 0)),
        13: lambda: relay(3, 1),
        15: lambda: arrive(4, 3),
    }

    @pl.loop(0, steps)
    def _(t):
        for when, event in events.items():
            @pl.when(t == when)
            def _():
                event()

        @pl.when(t + 1 < steps)
        def _():
            pair_load(t + 1).start()
        pair_load(t).wait()

        @pl.when(t >= 2)
        def _():
            out_put(t - 2).wait()
        slot = lax.rem(t, 2)
        group = lax.rem(t, 8)

        def emit(i, value):
            obuf[slot, i] = pbuf[slot, i] + value

        multiply(left_vm.at[group], keep_vm[pl.ds(pl.multiple_of(group * I_STEP, I_STEP), I_STEP), :], bvm.at[t // 8],
                 lift, bias, outer, scale, emit)
        out_put(t).start()

    relay(3, 2)
    relay(3, 3)
    settle(2)
    settle(3)
    out_put(steps - 2).wait()
    out_put(steps - 1).wait()
    for export in exports:
        export.wait()
    for swap in swaps:
        swap.wait_send()
    for item in range(blocks + 1):
        for h in range(1, 4):
            for way in range(2):
                @pl.when(out_ok(way, h))
                def _():
                    z_send(item, way, h).wait_send()
    for q in range(blocks):
        for plane in range(4):
            y_send(q, plane, False).wait_send()
            for which in range(2):
                c_send(q, plane, which, False).wait_send()


def exchange(both, lift, bias, pair):
    _, blocks, chans, seqs, cols = both.shape
    rows, _, _, width = pair.shape
    src = 16
    total = src * seqs
    vmem = pl.BlockSpec(memory_space=pltpu.VMEM)
    hbm = pl.BlockSpec(memory_space=pl.ANY)
    dma = pltpu.SemaphoreType.DMA
    groups = rows // I_STEP
    hidden = chans - 1
    return pl.pallas_call(
        exchange_kernel,
        in_specs=[hbm, vmem, vmem, hbm],
        out_specs=[hbm] * 5,
        out_shape=[
            jax.ShapeDtypeStruct((rows, EARLY, cols, width), F32),
            jax.ShapeDtypeStruct((blocks, src, chans, seqs, cols), BF16),
            jax.ShapeDtypeStruct((4, 4, chans, seqs, cols), BF16),
            jax.ShapeDtypeStruct((groups, I_STEP * hidden, total), BF16),
            jax.ShapeDtypeStruct((rows, total), BF16),
        ],
        scratch_shapes=[
            pltpu.VMEM((groups, I_STEP * hidden, total), BF16),
            pltpu.VMEM((rows, total), BF16),
            pltpu.VMEM((hidden, rows, 4 * seqs), F32),
            pltpu.VMEM((4, chans, seqs, cols), BF16),
            pltpu.VMEM((2, src, chans, seqs, cols), BF16),
            pltpu.VMEM((I_STEP // 2, hidden * hidden, 2 * cols), BF16),
            pltpu.VMEM((I_STEP, cols), F32),
            pltpu.VMEM((2, I_STEP, cols, width), F32),
            pltpu.VMEM((2, I_STEP, cols, width), F32),
            pltpu.VMEM((blocks + 1, chans, seqs, cols), BF16),
            dma((2, 5, 3)), dma((2, 5, 3)), dma((4, 4)), dma((4, 4)), dma((4, 4, 2)), dma((4, 4, 2)),
            dma((3,)), dma((3,)), dma((5,)), dma, dma((2,)), dma((2,)), dma((2,)), dma((2,)),
        ],
        compiler_params=pltpu.CompilerParams(vmem_limit_bytes=VMEM_LIMIT, collective_id=0, has_side_effects=True),
        name='exchange',
    )(both, lift, bias, pair)


def finish_kernel(left_ref, keep_ref, right_ref, weight_ref, bias_ref, pair_ref, early_ref, out_ref, outer_ref, scale_ref):
    out_ref[:, 0] = early_ref[...]

    def emit(i, value):
        out_ref[i, 1] = pair_ref[i] + value

    multiply(left_ref, keep_ref[...], right_ref, weight_ref, bias_ref, outer_ref, scale_ref, emit)


def finish(left, keep, right, weight, bias, pair, early):
    groups, depth, total = left.shape
    blocks, src, chans, seqs, cols = right.shape
    rows, _, _, width = pair.shape
    hidden = chans - 1
    pair = pair.reshape(rows, 2, EARLY, cols, width)
    out = pl.pallas_call(
        finish_kernel,
        grid=(blocks - EARLY, groups),
        in_specs=[
            pl.BlockSpec((None, depth, total), lambda q, g: (g, 0, 0)),
            pl.BlockSpec((I_STEP, total), lambda q, g: (g, 0)),
            pl.BlockSpec((None, src, chans, seqs, cols), lambda q, g: (q + EARLY, 0, 0, 0, 0)),
            pl.BlockSpec(weight.shape, lambda q, g: (0, 0)),
            pl.BlockSpec(bias.shape, lambda q, g: (0, 0)),
            pl.BlockSpec((I_STEP, None, None, cols, width), lambda q, g: (g, 1, q, 0, 0)),
            pl.BlockSpec((I_STEP, None, cols, width), lambda q, g: (g, q, 0, 0)),
        ],
        out_specs=pl.BlockSpec((I_STEP, 2, None, cols, width), lambda q, g: (g, 0, q, 0, 0)),
        out_shape=jax.ShapeDtypeStruct(pair.shape, F32),
        scratch_shapes=[pltpu.VMEM((I_STEP // 2, hidden * hidden, 2 * cols), BF16), pltpu.VMEM((I_STEP, cols), F32)],
        compiler_params=pltpu.CompilerParams(vmem_limit_bytes=VMEM_LIMIT),
        name='finish',
    )(left, keep, right, weight, bias, pair, early)
    return out.reshape(rows, blocks * cols, width)


def solution(mesh):
    msa_spec = P(('data', 'seq', 'dap'), None, None)
    mask_spec = P(('data', 'seq', 'dap'), None)
    pair_spec = P(('data', 'dap'), None, None)

    def device_step(msa, mask, pair, ln_gamma, ln_beta, w_a, b_a, w_b, b_b, w_out, b_out):
        hidden = w_a.shape[1]
        width = w_out.shape[1]
        res = msa.shape[1]
        weight = jnp.concatenate([w_a, w_b], axis=1).T
        bias = jnp.concatenate([b_a, b_b]).astype(F32)[:, None]
        both = project(msa, mask, ln_gamma.astype(F32)[:, None], ln_beta.astype(F32)[:, None], weight, bias)
        lift = w_out.reshape(hidden, hidden, width).transpose(2, 1, 0).reshape(width, hidden * hidden)
        bias_col = jnp.broadcast_to(b_out.astype(F32)[:, None], (width, J_STEP))
        tiled = pair.reshape(pair.shape[0], res // J_STEP, J_STEP, width)
        early, right, _, left, keep = exchange(both, lift, bias_col, tiled)
        return finish(left, keep, right, lift, bias_col, tiled, early)

    return jax.shard_map(device_step, mesh=mesh, in_specs=(msa_spec, mask_spec, pair_spec, P(), P(), P(), P(), P(), P(), P(), P()), out_specs=pair_spec, check_vma=False)
```

```python
import functools
import jax
import jax.numpy as jnp
from jax import lax
from jax.sharding import PartitionSpec as P
from jax.experimental import pallas as pl
from jax.experimental.pallas import tpu as pltpu

F32 = jnp.float32
BF16 = jnp.bfloat16
VMEM_LIMIT = 60 * 1024 * 1024
S_STEP = 16
I_STEP = 16
J_STEP = 128
MESH = pl.DeviceIdType.MESH
ITEMS = ('b0', 'b1', 'a0', 'a1', 'a2', 'b2', 'b3', 'a3')
EARLY = 2


def project_kernel(msa_ref, mask_ref, vec_ref, weight_ref, out_ref, tmp_ref):
    width = msa_ref.shape[1]
    for s in range(S_STEP):
        x = msa_ref[s].astype(F32)
        mean = jnp.sum(x, axis=0, keepdims=True) * (1.0 / width)
        centered = x - mean
        var = jnp.sum(centered * centered, axis=0, keepdims=True) * (1.0 / width)
        normed = centered * lax.rsqrt(var + 1e-5)
        normed = (normed * vec_ref[:, 0:1] + vec_ref[:, 1:2]).astype(BF16)
        proj = jnp.dot(weight_ref[...], normed, preferred_element_type=F32) + vec_ref[:, 2:3]
        tmp_ref[s] = proj * mask_ref[s:s + 1, :].astype(F32)
    half = out_ref.shape[2] - 1
    for g in range(2 * half // 8):
        flat = jnp.transpose(tmp_ref[:, g * 8:g * 8 + 8, :], (1, 0, 2)).astype(BF16)
        part, base = divmod(g * 8, half)
        for k in range(out_ref.shape[1]):
            out_ref[part, k, base:base + 8] = flat[:, :, k * J_STEP:(k + 1) * J_STEP]
    keep = mask_ref[...].astype(F32).astype(BF16)
    for k in range(out_ref.shape[1]):
        out_ref[0, k, half] = keep[:, k * J_STEP:(k + 1) * J_STEP]
        out_ref[1, k, half] = keep[:, k * J_STEP:(k + 1) * J_STEP]


def project(msa, mask, vec, weight):
    seqs, width, res = msa.shape
    chans = weight.shape[0]
    return pl.pallas_call(
        project_kernel,
        grid=(seqs // S_STEP,),
        in_specs=[
            pl.BlockSpec((S_STEP, width, res), lambda g: (g, 0, 0)),
            pl.BlockSpec((S_STEP, res), lambda g: (g, 0)),
            pl.BlockSpec((width, 3), lambda g: (0, 0)),
            pl.BlockSpec((chans, width), lambda g: (0, 0)),
        ],
        out_specs=pl.BlockSpec((2, res // J_STEP, chans // 2 + 1, S_STEP, J_STEP), lambda g: (0, 0, 0, g, 0)),
        out_shape=jax.ShapeDtypeStruct((2, res // J_STEP, chans // 2 + 1, seqs, J_STEP), BF16),
        scratch_shapes=[pltpu.VMEM((S_STEP, chans, res), F32)],
        compiler_params=pltpu.CompilerParams(vmem_limit_bytes=VMEM_LIMIT),
        name='project',
    )(msa, mask, vec, weight)


def multiply(left, spot, right, weight, bias, outer_ref, scale_ref, emit):
    src, chans, seqs, cols = right.shape
    chans = chans - 1
    total = src * seqs
    rows = I_STEP

    def rows_of(start, size):
        return jnp.concatenate([left[p, pl.ds(start, size), :] for p in range(left.shape[0])], axis=1)

    base = pl.multiple_of(spot * (rows * chans), rows * chans)
    keep = rows_of(pl.multiple_of(2 * rows * chans + spot * rows, rows), rows)
    count = jnp.dot(keep, right[:, chans].reshape(total, cols), preferred_element_type=F32)
    scale_ref[...] = 1.0 / (1e-3 + count)
    for g in range(chans // 4):
        slab = [right[:, g * 4 + k].reshape(total, cols) for k in range(4)]
        rhs = jnp.concatenate(slab, axis=1)
        for m in range(rows // 8):
            part = rows_of(pl.multiple_of(base + m * 8 * chans, 8 * chans), 8 * chans)
            prod = jnp.dot(part, rhs, preferred_element_type=F32).astype(BF16)
            for k in range(4):
                at = (g * 4 + k) * chans
                for i in range(8):
                    outer_ref[m * 4 + i // 2, at:at + chans, (i % 2) * cols:(i % 2 + 1) * cols] = (
                        prod[i * chans:(i + 1) * chans, k * cols:(k + 1) * cols])
    for h in range(rows // 2):
        lifted = jnp.dot(weight[...], outer_ref[h], preferred_element_type=F32)
        for k in range(2):
            part = lifted[:, k * cols:(k + 1) * cols] + bias[...]
            part = part * scale_ref[h * 2 + k:h * 2 + k + 1, :]
            emit(h * 2 + k, part.T)


def exchange_kernel(both, lift, bias, pair, x_out, right_out, left_out,
                    left_vm, right_vm, tmp, araw, outer, scale, pbuf, obuf,
                    zs, zr, ys, yr, cs, cr, ss, sr, ls, psem, osem, esem):
    z = lax.axis_index('seq')
    dap = lax.axis_index('dap')
    core = dap + 1 - 2 * lax.rem(dap, 2)
    far = lax.rem(dap + 2, 4)
    diag = lax.rem(core + 2, 4)
    me = z * 4 + dap
    blocks = both.shape[1]

    def remote(src, dst, send, recv, **target):
        return pltpu.make_async_remote_copy(src_ref=src, dst_ref=dst, send_sem=send, recv_sem=recv,
                                            device_id=target, device_id_type=MESH)

    def piece(item, plane):
        kind, at = ITEMS[item][0], int(ITEMS[item][1])
        return left_vm.at[at, plane] if kind == 'a' else right_vm.at[at, plane * 4 + dap]

    def out_ok(way, h):
        return (z < 3) & (z >= h - 1) if way == 0 else (z > 0) & (z <= 4 - h)

    def in_ok(way, h):
        return z >= h if way == 0 else z + h <= 3

    def z_send(item, way, h):
        sign = 1 - 2 * way
        at = piece(item, z - sign * (h - 1))
        return remote(at, at, zs.at[way, item, h - 1], zr.at[way, item, h - 1], seq=z + sign)

    def z_land(item, way, h):
        sign = 1 - 2 * way
        at = piece(item, z - sign * h)
        return remote(at, at, zs.at[way, item, h - 1], zr.at[way, item, h - 1], seq=z - sign)

    def y_copy(q, plane, owner):
        at = right_vm.at[q, plane * 4 + owner]
        return remote(at, at, ys.at[q, plane], yr.at[q, plane], dap=far)

    def c_copy(q, plane, which, owner):
        at = right_vm.at[q, plane * 4 + owner]
        return remote(at, at, cs.at[q, plane, which], cr.at[q, plane, which], dap=core)

    def begin(item):
        for way in range(2):
            @pl.when(out_ok(way, 1))
            def _():
                if item > 0:
                    z_send(item - 1, way, 1).wait_send()
                z_send(item, way, 1).start()
        if ITEMS[item][0] == 'b':
            q = int(ITEMS[item][1])
            y_copy(q, z, dap).start()
            c_copy(q, z, 0, dap).start()

    def early(item, *hops):
        for h in hops:
            for way in range(2):
                @pl.when(in_ok(way, h) & out_ok(way, h + 1))
                def _():
                    z_land(item, way, h).wait_recv()
                    z_send(item, way, h + 1).start()

    def late(item, *hops):
        for h in hops:
            for way in range(2):
                end = z == (3 if way == 0 else 0)

                @pl.when(in_ok(way, h) & end)
                def _():
                    z_land(item, way, h).wait_recv()

                if ITEMS[item][0] == 'b':
                    @pl.when(in_ok(way, h))
                    def _():
                        q = int(ITEMS[item][1])
                        plane = z - (1 - 2 * way) * h
                        y_copy(q, plane, dap).start()
                        c_copy(q, plane, 0, dap).start()

    def relay(q, *hops):
        for h in hops:
            if h == 0:
                y_copy(q, z, far).wait_recv()
                c_copy(q, z, 1, far).start()
            else:
                for way in range(2):
                    @pl.when(in_ok(way, h))
                    def _():
                        plane = z - (1 - 2 * way) * h
                        y_copy(q, plane, far).wait_recv()
                        c_copy(q, plane, 1, far).start()

    def export(q):
        return pltpu.make_async_copy(right_vm.at[q], right_out.at[q - EARLY], esem.at[q])

    def settle(q):
        for plane in range(4):
            for which, owner in enumerate((core, diag)):
                c_copy(q, plane, which, owner).wait_recv()
        if q >= EARLY:
            export(q).start()

    def turn():
        chans = araw.shape[1]
        for c in range(chans):
            block = araw[:, c].reshape(128, 128).astype(F32).T
            if c == chans - 1:
                for r in range(blocks):
                    left_vm[r, z, 1024:1056, :] = block[r * 32:(r + 1) * 32].astype(BF16)
            else:
                tmp[c] = block

        @pl.loop(0, 16)
        def _(k):
            start = pl.multiple_of(k * 8, 8)
            block = jnp.transpose(tmp[:, pl.ds(start, 8), :], (1, 0, 2)).reshape(256, 128)
            row = pl.multiple_of(lax.rem(k, 4) * 256, 256)
            left_vm[k // 4, z, pl.ds(row, 256), :] = block.astype(BF16)

    barrier = pltpu.get_barrier_semaphore()
    for other in (core, far, diag):
        pl.semaphore_signal(barrier, inc=1, device_id={'dap': other}, device_id_type=MESH)
    for way in range(2):
        @pl.when(out_ok(way, 1))
        def _():
            pl.semaphore_signal(barrier, inc=1, device_id={'seq': z + 1 - 2 * way}, device_id_type=MESH)
    inner = (z > 0) & (z < 3)
    loads = [pltpu.make_async_copy(both.at[1, q], right_vm.at[q, me], ls.at[q]) for q in range(blocks)]
    loads.append(pltpu.make_async_copy(both.at[0, dap], araw.at[dap], ls.at[blocks]))
    for load in loads:
        load.start()

    @pl.when(inner)
    def _():
        pl.semaphore_wait(barrier, 5)

    @pl.when(jnp.logical_not(inner))
    def _():
        pl.semaphore_wait(barrier, 4)

    swaps = [remote(both.at[0, other], araw.at[dap], ss.at[k], sr.at[k], dap=other)
             for k, other in enumerate((core, far, diag))]
    for k in (1, 2, 0):
        swaps[k].start()
    for load in loads:
        load.wait()
    begin(0)
    for k, other in enumerate((core, far, diag)):
        remote(araw.at[other], araw.at[other], ss.at[k], sr.at[k], dap=other).wait_recv()
    begin(1)
    turn()
    early(0, 1, 2)
    begin(2)
    late(0, 1, 2)
    relay(0, 0, 1)
    early(1, 1, 2)
    begin(3)
    late(0, 3)
    relay(0, 2, 3)
    late(1, 1, 2)
    relay(1, 0, 1)
    early(2, 1, 2)
    begin(4)
    late(1, 3)
    relay(1, 2, 3)
    settle(0)
    settle(1)
    late(2, 1, 2, 3)

    steps = 8 * EARLY
    final = pltpu.make_async_copy(left_vm, left_out, esem.at[blocks])

    def part(t):
        return t // (2 * EARLY)

    def col(t):
        return lax.rem(t, 2 * EARLY) // 2

    def tile(t):
        row = (part(t) * 2 + lax.rem(t, 2)) * I_STEP
        return pl.ds(pl.multiple_of(row, I_STEP), I_STEP), col(t)

    def pair_load(t):
        slot = lax.rem(t, 2)
        return pltpu.make_async_copy(pair.at[tile(t)], pbuf.at[slot], psem.at[slot])

    def out_put(t):
        slot = lax.rem(t, 2)
        return pltpu.make_async_copy(obuf.at[slot], x_out.at[tile(t)], osem.at[slot])

    pair_load(jnp.int32(0)).start()
    events = {
        0: lambda: early(3, 1),
        2: lambda: (early(3, 2), begin(5)),
        4: lambda: (late(3, 1, 2, 3), early(4, 1)),
        6: lambda: (early(4, 2), begin(6)),
        8: lambda: (late(4, 1, 2, 3), early(5, 1), late(5, 1)),
        9: lambda: (begin(7), relay(2, 0)),
        10: lambda: (early(5, 2), late(5, 2), early(6, 1), relay(2, 1)),
        11: lambda: late(6, 1),
        12: lambda: (early(6, 2), late(5, 3), late(6, 2), early(7, 1), relay(2, 2), relay(3, 0), early(7, 2),
                     late(6, 3), relay(2, 3), settle(2), relay(3, 1), late(7, 1, 2, 3), final.start()),
        13: lambda: relay(3, 2),
        14: lambda: (relay(3, 3), settle(3)),
    }

    @pl.loop(0, steps)
    def _(t):
        for when, event in events.items():
            @pl.when(t == when)
            def _():
                event()

        @pl.when(t + 1 < steps)
        def _():
            pair_load(t + 1).start()
        pair_load(t).wait()

        @pl.when(t >= 2)
        def _():
            out_put(t - 2).wait()
        slot = lax.rem(t, 2)

        def emit(i, value):
            obuf[slot, i] = pbuf[slot, i] + value

        multiply(left_vm.at[part(t)], lax.rem(t, 2), right_vm.at[col(t)], lift, bias, outer, scale, emit)
        out_put(t).start()

    out_put(jnp.int32(steps - 2)).wait()
    out_put(jnp.int32(steps - 1)).wait()
    for q in range(EARLY, blocks):
        export(q).wait()
    final.wait()
    for swap in swaps:
        swap.wait_send()
    for item in range(len(ITEMS)):
        for h in range(1 if item == len(ITEMS) - 1 else 2, 4):
            for way in range(2):
                @pl.when(out_ok(way, h))
                def _():
                    z_send(item, way, h).wait_send()
    for q in range(blocks):
        for plane in range(4):
            y_copy(q, plane, dap).wait_send()
            for which, owner in enumerate((dap, far)):
                c_copy(q, plane, which, owner).wait_send()


def exchange(both, lift, bias, pair):
    _, blocks, chans, seqs, cols = both.shape
    rows, _, _, width = pair.shape
    src = 16
    vmem = pl.BlockSpec(memory_space=pltpu.VMEM)
    hbm = pl.BlockSpec(memory_space=pl.ANY)
    dma = pltpu.SemaphoreType.DMA
    hidden = chans - 1
    part = rows // blocks
    left_shape = (4, part * hidden + part, 4 * seqs)
    return pl.pallas_call(
        exchange_kernel,
        in_specs=[hbm, vmem, vmem, hbm],
        out_specs=[hbm] * 3,
        out_shape=[
            jax.ShapeDtypeStruct((rows, EARLY, cols, width), F32),
            jax.ShapeDtypeStruct((blocks - EARLY, src, chans, seqs, cols), BF16),
            jax.ShapeDtypeStruct((blocks,) + left_shape, BF16),
        ],
        scratch_shapes=[
            pltpu.VMEM((blocks,) + left_shape, BF16),
            pltpu.VMEM((blocks, src, chans, seqs, cols), BF16),
            pltpu.VMEM((hidden, rows, 4 * seqs), F32),
            pltpu.VMEM((4, chans, seqs, cols), BF16),
            pltpu.VMEM((I_STEP // 2, hidden * hidden, 2 * cols), BF16),
            pltpu.VMEM((I_STEP, cols), F32),
            pltpu.VMEM((2, I_STEP, cols, width), F32),
            pltpu.VMEM((2, I_STEP, cols, width), F32),
            dma((2, 8, 3)), dma((2, 8, 3)), dma((4, 4)), dma((4, 4)), dma((4, 4, 2)), dma((4, 4, 2)),
            dma((3,)), dma((3,)), dma((5,)), dma((2,)), dma((2,)), dma((5,)),
        ],
        compiler_params=pltpu.CompilerParams(vmem_limit_bytes=VMEM_LIMIT, collective_id=0, has_side_effects=True),
        name='exchange',
    )(both, lift, bias, pair)


def finish_kernel(left_ref, right_ref, weight_ref, bias_ref, pair_ref, early_ref, out_ref, outer_ref, scale_ref):
    out_ref[:, 0] = early_ref[...]

    def emit(i, value):
        out_ref[i, 1] = pair_ref[i] + value

    multiply(left_ref, lax.rem(pl.program_id(1), 2), right_ref, weight_ref, bias_ref, outer_ref, scale_ref, emit)


def finish(left, right, weight, bias, pair, early):
    rest, src, chans, seqs, cols = right.shape
    rows, blocks, _, width = pair.shape
    hidden = chans - 1
    pair = pair.reshape(rows, 2, EARLY, cols, width)
    out = pl.pallas_call(
        finish_kernel,
        grid=(rest, rows // I_STEP),
        in_specs=[
            pl.BlockSpec((None,) + left.shape[1:], lambda q, g: (g // 2, 0, 0, 0)),
            pl.BlockSpec((None, src, chans, seqs, cols), lambda q, g: (q, 0, 0, 0, 0)),
            pl.BlockSpec(weight.shape, lambda q, g: (0, 0)),
            pl.BlockSpec(bias.shape, lambda q, g: (0, 0)),
            pl.BlockSpec((I_STEP, None, None, cols, width), lambda q, g: (g, 1, q, 0, 0)),
            pl.BlockSpec((I_STEP, None, cols, width), lambda q, g: (g, q, 0, 0)),
        ],
        out_specs=pl.BlockSpec((I_STEP, 2, None, cols, width), lambda q, g: (g, 0, q, 0, 0)),
        out_shape=jax.ShapeDtypeStruct(pair.shape, F32),
        scratch_shapes=[pltpu.VMEM((I_STEP // 2, hidden * hidden, 2 * cols), BF16), pltpu.VMEM((I_STEP, cols), F32)],
        compiler_params=pltpu.CompilerParams(vmem_limit_bytes=VMEM_LIMIT),
        name='finish',
    )(left, right, weight, bias, pair, early)
    return out.reshape(rows, blocks * cols, width)


def solution(mesh):
    msa_spec = P(('data', 'seq', 'dap'), None, None)
    mask_spec = P(('data', 'seq', 'dap'), None)
    pair_spec = P(('data', 'dap'), None, None)

    def device_step(msa, mask, pair, ln_gamma, ln_beta, w_a, b_a, w_b, b_b, w_out, b_out):
        hidden = w_a.shape[1]
        width = w_out.shape[1]
        res = msa.shape[1]
        weight = jnp.concatenate([w_a.T, w_b.T], axis=0)
        vec = jnp.stack([ln_gamma, ln_beta, jnp.concatenate([b_a, b_b])], axis=1).astype(F32)
        both = project(msa.transpose(0, 2, 1), mask, vec, weight)
        lift = w_out.reshape(hidden, hidden, width).transpose(2, 1, 0).reshape(width, hidden * hidden)
        bias_col = jnp.broadcast_to(b_out.astype(F32)[:, None], (width, J_STEP))
        tiled = pair.reshape(pair.shape[0], res // J_STEP, J_STEP, width)
        early, right, left = exchange(both, lift, bias_col, tiled)
        return finish(left, right, lift, bias_col, tiled, early)

    return jax.shard_map(device_step, mesh=mesh, in_specs=(msa_spec, mask_spec, pair_spec, P(), P(), P(), P(), P(), P(), P(), P()), out_specs=pair_spec, check_vma=False)
```

```python
import functools
import jax
import jax.numpy as jnp
from jax import lax
from jax.sharding import PartitionSpec as P
from jax.experimental import pallas as pl
from jax.experimental.pallas import tpu as pltpu

F32 = jnp.float32
BF16 = jnp.bfloat16
VMEM_LIMIT = 60 * 1024 * 1024
S_STEP = 16
I_STEP = 16
J_STEP = 128
MESH = pl.DeviceIdType.MESH
ITEMS = ('b0', 'b1', 'a0', 'a1', 'a2', 'b2', 'b3', 'a3')
EARLY = 2


def project_kernel(msa_ref, mask_ref, vec_ref, weight_ref, out_ref, tmp_ref):
    width = msa_ref.shape[1]
    for s in range(S_STEP):
        x = msa_ref[s].astype(F32)
        mean = jnp.sum(x, axis=0, keepdims=True) * (1.0 / width)
        centered = x - mean
        var = jnp.sum(centered * centered, axis=0, keepdims=True) * (1.0 / width)
        normed = centered * lax.rsqrt(var + 1e-5)
        normed = (normed * vec_ref[:, 0:1] + vec_ref[:, 1:2]).astype(BF16)
        proj = jnp.dot(weight_ref[...], normed, preferred_element_type=F32) + vec_ref[:, 2:3]
        tmp_ref[s] = proj * mask_ref[s:s + 1, :].astype(F32)
    half = out_ref.shape[2] - 1
    for g in range(2 * half // 8):
        flat = jnp.transpose(tmp_ref[:, g * 8:g * 8 + 8, :], (1, 0, 2)).astype(BF16)
        part, base = divmod(g * 8, half)
        for k in range(out_ref.shape[1]):
            out_ref[part, k, base:base + 8] = flat[:, :, k * J_STEP:(k + 1) * J_STEP]
    keep = mask_ref[...].astype(F32).astype(BF16)
    for k in range(out_ref.shape[1]):
        out_ref[0, k, half] = keep[:, k * J_STEP:(k + 1) * J_STEP]
        out_ref[1, k, half] = keep[:, k * J_STEP:(k + 1) * J_STEP]


def project(msa, mask, vec, weight):
    seqs, width, res = msa.shape
    chans = weight.shape[0]
    return pl.pallas_call(
        project_kernel,
        grid=(seqs // S_STEP,),
        in_specs=[
            pl.BlockSpec((S_STEP, width, res), lambda g: (g, 0, 0)),
            pl.BlockSpec((S_STEP, res), lambda g: (g, 0)),
            pl.BlockSpec((width, 3), lambda g: (0, 0)),
            pl.BlockSpec((chans, width), lambda g: (0, 0)),
        ],
        out_specs=pl.BlockSpec((2, res // J_STEP, chans // 2 + 1, S_STEP, J_STEP), lambda g: (0, 0, 0, g, 0)),
        out_shape=jax.ShapeDtypeStruct((2, res // J_STEP, chans // 2 + 1, seqs, J_STEP), BF16),
        scratch_shapes=[pltpu.VMEM((S_STEP, chans, res), F32)],
        compiler_params=pltpu.CompilerParams(vmem_limit_bytes=VMEM_LIMIT),
        name='project',
    )(msa, mask, vec, weight)


def multiply(left, spot, right, weight, bias, outer_ref, scale_ref, emit):
    src, chans, seqs, cols = right.shape
    chans = chans - 1
    total = src * seqs
    rows = I_STEP

    def rows_of(start, size):
        return jnp.concatenate([left[p, pl.ds(start, size), :] for p in range(left.shape[0])], axis=1)

    base = pl.multiple_of(spot * (rows * chans), rows * chans)
    keep = rows_of(pl.multiple_of(2 * rows * chans + spot * rows, rows), rows)
    count = jnp.dot(keep, right[:, chans].reshape(total, cols), preferred_element_type=F32)
    scale_ref[...] = 1.0 / (1e-3 + count)
    column = jnp.broadcast_to(bias[...].astype(F32), (cols, bias.shape[1])).T
    for g in range(chans // 4):
        slab = [right[:, g * 4 + k].reshape(total, cols) for k in range(4)]
        rhs = jnp.concatenate(slab, axis=1)
        for m in range(rows // 8):
            part = rows_of(pl.multiple_of(base + m * 8 * chans, 8 * chans), 8 * chans)
            prod = jnp.dot(part, rhs, preferred_element_type=F32).astype(BF16)
            for k in range(4):
                at = (g * 4 + k) * chans
                for i in range(8):
                    outer_ref[m * 4 + i // 2, at:at + chans, (i % 2) * cols:(i % 2 + 1) * cols] = (
                        prod[i * chans:(i + 1) * chans, k * cols:(k + 1) * cols])
    for h in range(rows // 2):
        lifted = jnp.dot(weight[...], outer_ref[h], preferred_element_type=F32)
        for k in range(2):
            part = lifted[:, k * cols:(k + 1) * cols] + column
            part = part * scale_ref[h * 2 + k:h * 2 + k + 1, :]
            emit(h * 2 + k, part.T)


def exchange_kernel(both, lift, bias, pair, x_out, right_out, left_out,
                    left_vm, right_vm, tmp, araw, outer, scale, pbuf, obuf,
                    zs, zr, ys, yr, cs, cr, ss, sr, ls, psem, osem, esem):
    z = lax.axis_index('seq')
    dap = lax.axis_index('dap')
    core = dap + 1 - 2 * lax.rem(dap, 2)
    far = lax.rem(dap + 2, 4)
    diag = lax.rem(core + 2, 4)
    me = z * 4 + dap
    blocks = both.shape[1]

    def remote(src, dst, send, recv, **target):
        return pltpu.make_async_remote_copy(src_ref=src, dst_ref=dst, send_sem=send, recv_sem=recv,
                                            device_id=target, device_id_type=MESH)

    def piece(item, plane):
        kind, at = ITEMS[item][0], int(ITEMS[item][1])
        return left_vm.at[at, plane] if kind == 'a' else right_vm.at[at, plane * 4 + dap]

    def out_ok(way, h):
        return (z < 3) & (z >= h - 1) if way == 0 else (z > 0) & (z <= 4 - h)

    def in_ok(way, h):
        return z >= h if way == 0 else z + h <= 3

    def z_send(item, way, h):
        sign = 1 - 2 * way
        at = piece(item, z - sign * (h - 1))
        return remote(at, at, zs.at[way, item, h - 1], zr.at[way, item, h - 1], seq=z + sign)

    def z_land(item, way, h):
        sign = 1 - 2 * way
        at = piece(item, z - sign * h)
        return remote(at, at, zs.at[way, item, h - 1], zr.at[way, item, h - 1], seq=z - sign)

    def y_copy(q, plane, owner):
        at = right_vm.at[q, plane * 4 + owner]
        return remote(at, at, ys.at[q, plane], yr.at[q, plane], dap=far)

    def c_copy(q, plane, which, owner):
        at = right_vm.at[q, plane * 4 + owner]
        return remote(at, at, cs.at[q, plane, which], cr.at[q, plane, which], dap=core)

    def begin(item):
        for way in range(2):
            @pl.when(out_ok(way, 1))
            def _():
                if item > 0:
                    z_send(item - 1, way, 1).wait_send()
                z_send(item, way, 1).start()
        if ITEMS[item][0] == 'b':
            q = int(ITEMS[item][1])
            y_copy(q, z, dap).start()
            c_copy(q, z, 0, dap).start()

    def early(item, *hops):
        for h in hops:
            for way in range(2):
                @pl.when(in_ok(way, h) & out_ok(way, h + 1))
                def _():
                    z_land(item, way, h).wait_recv()
                    z_send(item, way, h + 1).start()

    def late(item, *hops):
        for h in hops:
            for way in range(2):
                end = z == (3 if way == 0 else 0)

                @pl.when(in_ok(way, h) & end)
                def _():
                    z_land(item, way, h).wait_recv()

                if ITEMS[item][0] == 'b':
                    @pl.when(in_ok(way, h))
                    def _():
                        q = int(ITEMS[item][1])
                        plane = z - (1 - 2 * way) * h
                        y_copy(q, plane, dap).start()
                        c_copy(q, plane, 0, dap).start()

    def relay(q, *hops):
        for h in hops:
            if h == 0:
                y_copy(q, z, far).wait_recv()
                c_copy(q, z, 1, far).start()
            else:
                for way in range(2):
                    @pl.when(in_ok(way, h))
                    def _():
                        plane = z - (1 - 2 * way) * h
                        y_copy(q, plane, far).wait_recv()
                        c_copy(q, plane, 1, far).start()

    def export(q):
        return pltpu.make_async_copy(right_vm.at[q], right_out.at[q - EARLY], esem.at[q])

    def settle(q):
        for plane in range(4):
            for which, owner in enumerate((core, diag)):
                c_copy(q, plane, which, owner).wait_recv()
        if q >= EARLY:
            export(q).start()

    def turn():
        chans = araw.shape[1]
        for c in range(chans):
            block = araw[:, c].reshape(128, 128).astype(F32).T
            if c == chans - 1:
                for r in range(blocks):
                    left_vm[r, z, 1024:1056, :] = block[r * 32:(r + 1) * 32].astype(BF16)
            else:
                tmp[c] = block

        @pl.loop(0, 16)
        def _(k):
            start = pl.multiple_of(k * 8, 8)
            block = jnp.transpose(tmp[:, pl.ds(start, 8), :], (1, 0, 2)).reshape(256, 128)
            row = pl.multiple_of(lax.rem(k, 4) * 256, 256)
            left_vm[k // 4, z, pl.ds(row, 256), :] = block.astype(BF16)

    barrier = pltpu.get_barrier_semaphore()
    for other in (core, far, diag):
        pl.semaphore_signal(barrier, inc=1, device_id={'dap': other}, device_id_type=MESH)
    for way in range(2):
        @pl.when(out_ok(way, 1))
        def _():
            pl.semaphore_signal(barrier, inc=1, device_id={'seq': z + 1 - 2 * way}, device_id_type=MESH)
    inner = (z > 0) & (z < 3)
    loads = [pltpu.make_async_copy(both.at[1, q], right_vm.at[q, me], ls.at[q]) for q in range(blocks)]
    loads.append(pltpu.make_async_copy(both.at[0, dap], araw.at[dap], ls.at[blocks]))
    for load in loads:
        load.start()

    @pl.when(inner)
    def _():
        pl.semaphore_wait(barrier, 5)

    @pl.when(jnp.logical_not(inner))
    def _():
        pl.semaphore_wait(barrier, 4)

    swaps = [remote(both.at[0, other], araw.at[dap], ss.at[k], sr.at[k], dap=other)
             for k, other in enumerate((core, far, diag))]
    for k in (1, 2, 0):
        swaps[k].start()
    for load in loads:
        load.wait()
    begin(0)
    for k, other in enumerate((core, far, diag)):
        remote(araw.at[other], araw.at[other], ss.at[k], sr.at[k], dap=other).wait_recv()
    begin(1)
    turn()
    early(0, 1, 2)
    begin(2)
    late(0, 1, 2)
    relay(0, 0, 1)
    early(1, 1, 2)
    begin(3)
    late(0, 3)
    relay(0, 2, 3)
    late(1, 1, 2)
    relay(1, 0, 1)
    early(2, 1, 2)
    begin(4)
    late(1, 3)
    relay(1, 2, 3)
    settle(0)
    settle(1)
    late(2, 1, 2, 3)

    steps = 8 * EARLY
    final = pltpu.make_async_copy(left_vm, left_out, esem.at[blocks])

    def part(t):
        return t // (2 * EARLY)

    def col(t):
        return lax.rem(t, 2 * EARLY) // 2

    def tile(t):
        row = (part(t) * 2 + lax.rem(t, 2)) * I_STEP
        return pl.ds(pl.multiple_of(row, I_STEP), I_STEP), col(t)

    def pair_load(t):
        slot = lax.rem(t, 2)
        return pltpu.make_async_copy(pair.at[tile(t)], pbuf.at[slot], psem.at[slot])

    def out_put(t):
        slot = lax.rem(t, 2)
        return pltpu.make_async_copy(obuf.at[slot], x_out.at[tile(t)], osem.at[slot])

    pair_load(jnp.int32(0)).start()
    events = {
        0: lambda: early(3, 1),
        2: lambda: (early(3, 2), begin(5)),
        4: lambda: (late(3, 1, 2, 3), early(4, 1)),
        6: lambda: (early(4, 2), begin(6)),
        8: lambda: (late(4, 1, 2, 3), early(5, 1), late(5, 1)),
        9: lambda: (begin(7), relay(2, 0)),
        10: lambda: (early(5, 2), late(5, 2), early(6, 1), relay(2, 1)),
        11: lambda: late(6, 1),
        12: lambda: (early(6, 2), late(5, 3), late(6, 2), early(7, 1), relay(2, 2), relay(3, 0), early(7, 2),
                     late(6, 3), relay(2, 3), settle(2), relay(3, 1), late(7, 1, 2, 3), final.start()),
        13: lambda: relay(3, 2),
        14: lambda: (relay(3, 3), settle(3)),
    }

    @pl.loop(0, steps)
    def _(t):
        for when, event in events.items():
            @pl.when(t == when)
            def _():
                event()

        @pl.when(t + 1 < steps)
        def _():
            pair_load(t + 1).start()
        pair_load(t).wait()

        @pl.when(t >= 2)
        def _():
            out_put(t - 2).wait()
        slot = lax.rem(t, 2)

        def emit(i, value):
            obuf[slot, i] = pbuf[slot, i] + value

        multiply(left_vm.at[part(t)], lax.rem(t, 2), right_vm.at[col(t)], lift, bias, outer, scale, emit)
        out_put(t).start()

    out_put(jnp.int32(steps - 2)).wait()
    out_put(jnp.int32(steps - 1)).wait()
    for q in range(EARLY, blocks):
        export(q).wait()
    final.wait()
    for swap in swaps:
        swap.wait_send()
    for item in range(len(ITEMS)):
        for h in range(1 if item == len(ITEMS) - 1 else 2, 4):
            for way in range(2):
                @pl.when(out_ok(way, h))
                def _():
                    z_send(item, way, h).wait_send()
    for q in range(blocks):
        for plane in range(4):
            y_copy(q, plane, dap).wait_send()
            for which, owner in enumerate((dap, far)):
                c_copy(q, plane, which, owner).wait_send()


def exchange(both, lift, bias, pair):
    _, blocks, chans, seqs, cols = both.shape
    rows, _, _, width = pair.shape
    src = 16
    vmem = pl.BlockSpec(memory_space=pltpu.VMEM)
    hbm = pl.BlockSpec(memory_space=pl.ANY)
    dma = pltpu.SemaphoreType.DMA
    hidden = chans - 1
    part = rows // blocks
    left_shape = (4, part * hidden + part, 4 * seqs)
    return pl.pallas_call(
        exchange_kernel,
        in_specs=[hbm, vmem, vmem, hbm],
        out_specs=[hbm] * 3,
        out_shape=[
            jax.ShapeDtypeStruct((rows, EARLY, cols, width), F32),
            jax.ShapeDtypeStruct((blocks - EARLY, src, chans, seqs, cols), BF16),
            jax.ShapeDtypeStruct((blocks,) + left_shape, BF16),
        ],
        scratch_shapes=[
            pltpu.VMEM((blocks,) + left_shape, BF16),
            pltpu.VMEM((blocks, src, chans, seqs, cols), BF16),
            pltpu.VMEM((hidden, rows, 4 * seqs), F32),
            pltpu.VMEM((4, chans, seqs, cols), BF16),
            pltpu.VMEM((I_STEP // 2, hidden * hidden, 2 * cols), BF16),
            pltpu.VMEM((I_STEP, cols), F32),
            pltpu.VMEM((2, I_STEP, cols, width), F32),
            pltpu.VMEM((2, I_STEP, cols, width), F32),
            dma((2, 8, 3)), dma((2, 8, 3)), dma((4, 4)), dma((4, 4)), dma((4, 4, 2)), dma((4, 4, 2)),
            dma((3,)), dma((3,)), dma((5,)), dma((2,)), dma((2,)), dma((5,)),
        ],
        compiler_params=pltpu.CompilerParams(vmem_limit_bytes=VMEM_LIMIT, collective_id=0, has_side_effects=True),
        name='exchange',
    )(both, lift, bias, pair)


def finish_kernel(left_ref, right_ref, weight_ref, bias_ref, pair_ref, early_ref, out_ref, outer_ref, scale_ref):
    out_ref[:, 0] = early_ref[...]

    def emit(i, value):
        out_ref[i, 1] = pair_ref[i] + value

    multiply(left_ref, lax.rem(pl.program_id(1), 2), right_ref, weight_ref, bias_ref, outer_ref, scale_ref, emit)


def finish(left, right, weight, bias, pair, early):
    rest, src, chans, seqs, cols = right.shape
    rows, blocks, _, width = pair.shape
    hidden = chans - 1
    pair = pair.reshape(rows, 2, EARLY, cols, width)
    out = pl.pallas_call(
        finish_kernel,
        grid=(rest, rows // I_STEP),
        in_specs=[
            pl.BlockSpec((None,) + left.shape[1:], lambda q, g: (g // 2, 0, 0, 0)),
            pl.BlockSpec((None, src, chans, seqs, cols), lambda q, g: (q, 0, 0, 0, 0)),
            pl.BlockSpec(weight.shape, lambda q, g: (0, 0)),
            pl.BlockSpec(bias.shape, lambda q, g: (0, 0)),
            pl.BlockSpec((I_STEP, None, None, cols, width), lambda q, g: (g, 1, q, 0, 0)),
            pl.BlockSpec((I_STEP, None, cols, width), lambda q, g: (g, q, 0, 0)),
        ],
        out_specs=pl.BlockSpec((I_STEP, 2, None, cols, width), lambda q, g: (g, 0, q, 0, 0)),
        out_shape=jax.ShapeDtypeStruct(pair.shape, F32),
        scratch_shapes=[pltpu.VMEM((I_STEP // 2, hidden * hidden, 2 * cols), BF16), pltpu.VMEM((I_STEP, cols), F32)],
        compiler_params=pltpu.CompilerParams(vmem_limit_bytes=VMEM_LIMIT),
        name='finish',
    )(left, right, weight, bias, pair, early)
    return out.reshape(rows, blocks * cols, width)


def solution(mesh):
    msa_spec = P(('data', 'seq', 'dap'), None, None)
    mask_spec = P(('data', 'seq', 'dap'), None)
    pair_spec = P(('data', 'dap'), None, None)

    def device_step(msa, mask, pair, ln_gamma, ln_beta, w_a, b_a, w_b, b_b, w_out, b_out):
        hidden = w_a.shape[1]
        width = w_out.shape[1]
        res = msa.shape[1]
        weight = jnp.concatenate([w_a.T, w_b.T], axis=0)
        vec = jnp.stack([ln_gamma, ln_beta, jnp.concatenate([b_a, b_b])], axis=1).astype(F32)
        both = project(msa.transpose(0, 2, 1), mask, vec, weight)
        lift = w_out.reshape(hidden, hidden, width).transpose(2, 1, 0).reshape(width, hidden * hidden)
        bias_col = b_out.reshape(1, width)
        tiled = pair.reshape(pair.shape[0], res // J_STEP, J_STEP, width)
        early, right, left = exchange(both, lift, bias_col, tiled)
        return finish(left, right, lift, bias_col, tiled, early)

    return jax.shard_map(device_step, mesh=mesh, in_specs=(msa_spec, mask_spec, pair_spec, P(), P(), P(), P(), P(), P(), P(), P()), out_specs=pair_spec, check_vma=False)
```
